16 devices in a mesh: rep: 1, dp: 16 (over x, y, z, core).
Axes of the slice: x: 2, y: 2, z: 2, core: 2. Of those that a mesh axis runs over, the one named last changes fastest.
Arguments:
- x: bfloat16 [16, 2048, 896], P(('rep', 'dp'))
- dy: bfloat16 [16, 2048, 896], P(('rep', 'dp'))
- w_gate: bfloat16 [2, 896, 2560], P(None, 'dp')
- w_up: bfloat16 [2, 896, 2560], P(None, 'dp')
- w_down: bfloat16 [2, 2560, 896], P(None, 'dp')
Outputs:
- output 1: bfloat16 [16, 2048, 896], P(('rep', 'dp'))
- output 2: bfloat16 [2, 896, 2560], P('rep', 'dp')
- output 3: bfloat16 [2, 896, 2560], P('rep', 'dp')
- output 4: bfloat16 [2, 2560, 896], P('rep', 'dp')
All inputs are finite; a program needn't handle non-finite values.
Results may differ from the reference program's by a relative error of at most 0.018.
Values are sent between devices in bfloat16 or wider.
A program may use at most 2 GiB of HBM per device.

```python
import jax
import jax.numpy as jnp
from jax import lax

SEQUENCES = 16
TOKENS = 2048
D = 896
FF = 2560
LAYERS = 2
NAMES = ("w_gate", "w_up", "w_down")
SHAPES = {"w_gate": (LAYERS, D, FF), "w_up": (LAYERS, D, FF), "w_down": (LAYERS, FF, D)}


def bump(key, n, height):
    away = (jnp.arange(n, dtype=jnp.int32) - jax.random.randint(key, (), 0, n, jnp.int32)) % n
    return jnp.where(away < n // 8, height, 1.0)


def together(key, own, strength):
    shared = jax.random.normal(key, own.shape[1:], jnp.float32)
    return (own + strength * shared) * lax.rsqrt(1 + strength * strength)


def setup_inputs(seed: int = 0, part: int = 0) -> dict:
    kx, kdy, ka, kb, kz, kf, kh, kl, *kw = jax.random.split(jax.random.key(seed), 8 + len(NAMES))
    kx, kdy, ka, kb = (jax.random.fold_in(k, part) for k in (kx, kdy, ka, kb))
    shape = (SEQUENCES, TOKENS, D)
    much_x, much_dy = jax.random.uniform(kz, (2,), jnp.float32, 0.0, 1.0)
    layers = 2.0 ** jax.random.uniform(kl, (LAYERS, 1, 1), jnp.float32, -1.0, 1.0)
    x = together(ka, jax.random.normal(kx, shape, jnp.float32), much_x) * bump(kf, D, 4.0)
    dy = together(kb, jax.random.normal(kdy, shape, jnp.float32), much_dy)
    drawn = {"x": x.astype(jnp.bfloat16), "dy": (dy * (SEQUENCES * TOKENS) ** -0.5).astype(jnp.bfloat16)}
    for key, name in zip(kw, NAMES, strict=True):
        w = jax.random.normal(key, SHAPES[name], jnp.float32) * SHAPES[name][1] ** -0.5
        drawn[name] = (w * {"w_gate": 1.0, "w_up": bump(kh, FF, 4.0), "w_down": layers}[name]).astype(jnp.bfloat16)
    return drawn


def matmul(a, w):
    return jnp.dot(a, w, preferred_element_type=jnp.float32).astype(jnp.bfloat16)


def normed(h):
    wide = h.astype(jnp.float32)
    scale = lax.rsqrt(jnp.mean(wide**2, -1, keepdims=True) + 1e-6)
    return (wide * scale).astype(jnp.bfloat16)


def layer(h, w):
    a = normed(h)
    gate = jnp.dot(a, w["w_gate"], preferred_element_type=jnp.float32)
    up = jnp.dot(a, w["w_up"], preferred_element_type=jnp.float32)
    return h + matmul((jax.nn.silu(gate) * up).astype(jnp.bfloat16), w["w_down"])


def stack(weights, h):
    return lax.scan(lambda h, w: (layer(h, w), None), h, weights)[0]


def reference(x, dy, w_gate, w_up, w_down):
    weights = dict(zip(NAMES, (w_gate, w_up, w_down), strict=True))

    def take(so_far, sequence):
        h, by_y = sequence
        _, back = jax.vjp(stack, weights, h)
        by_weights, by_h = back(by_y)
        return jax.tree.map(lambda total, term: total + term.astype(jnp.float32), so_far, by_weights), by_h

    none_yet = {name: jnp.zeros(w.shape, jnp.float32) for name, w in weights.items()}
    by_weights, by_x = lax.scan(take, none_yet, (x, dy))
    return (by_x, *(by_weights[name].astype(jnp.bfloat16) for name in NAMES))
```

```python
import jax
import jax.numpy as jnp
from jax import lax
from jax.sharding import PartitionSpec as P

NAMES = ("w_gate", "w_up", "w_down")


def dot(a, b, ca, cb):
    return lax.dot_general(a, b, (((ca,), (cb,)), ((), ())), preferred_element_type=jnp.float32)


def solution(mesh):
    def step(x, dy, w_gate, w_up, w_down):
        bf16, f32 = jnp.bfloat16, jnp.float32
        x, dy = x[0], dy[0]
        layers = w_gate.shape[0]
        full = [
            [lax.all_gather(w[l], "dp", axis=0, tiled=True) for w in (w_gate, w_up, w_down)] for l in range(layers)
        ]

        def normed(h):
            wide = h.astype(f32)
            scale = lax.rsqrt(jnp.mean(wide**2, -1, keepdims=True) + 1e-6)
            return (wide * scale).astype(bf16)

        h, kept = x, []
        for l in range(layers):
            wg, wu, wd = full[l]
            a = normed(h)
            gate = dot(a, wg, 1, 0)
            up = dot(a, wu, 1, 0)
            p = (jax.nn.silu(gate) * up).astype(bf16)
            kept.append((h, a, gate, up, p))
            if l + 1 < layers:
                h = h + dot(p, wd, 1, 0).astype(bf16)

        by_h, grads = dy, []
        for l in reversed(range(layers)):
            wg, wu, wd = full[l]
            h, a, gate, up, p = kept[l]
            by_p = dot(by_h, wd, 1, 1).astype(bf16)
            g_down = dot(p, by_h, 0, 0).astype(bf16)
            wide = by_p.astype(f32)
            sig = jax.nn.sigmoid(gate)
            d_up = (wide * (gate * sig)).astype(bf16)
            d_gate = (wide * up * (sig * (1 + gate * (1 - sig)))).astype(bf16)
            g_gate = dot(a, d_gate, 0, 0).astype(bf16)
            g_up = dot(a, d_up, 0, 0).astype(bf16)
            by_a = dot(d_gate, wg, 1, 1).astype(bf16) + dot(d_up, wu, 1, 1).astype(bf16)
            _, back = jax.vjp(normed, h)
            by_h = by_h + back(by_a)[0]
            grads.append([lax.psum_scatter(g, "dp", scatter_dimension=0, tiled=True) for g in (g_gate, g_up, g_down)])
        grads = grads[::-1]
        outs = [jnp.stack([grads[l][i] for l in range(layers)]) for i in range(3)]
        return (by_h[None], *outs)

    tok = P(("rep", "dp"), None, None)
    w = P(None, "dp", None)
    g = P("rep", "dp", None)
    return jax.shard_map(step, mesh=mesh, in_specs=(tok, tok, w, w, w), out_specs=(tok, g, g, g), check_vma=False)
```

```python
import functools

import jax
import jax.numpy as jnp
from jax import lax
from jax.experimental import pallas as pl
from jax.experimental.pallas import tpu as pltpu
from jax.sharding import PartitionSpec as P

bf16, f32 = jnp.bfloat16, jnp.float32
MESH = pl.DeviceIdType.MESH
ANY = pl.BlockSpec(memory_space=pl.ANY)
MIB = 1 << 20
CORE, Z, Y, X = 1, 2, 4, 8
ORDERS = ((X, Y, Z), (Y, Z, X), (Z, X, Y))


def thirds(columns):
    tiles = columns // 128
    cuts = [0, (tiles + 2) // 3, (tiles + 2) // 3 + (tiles + 1) // 3, tiles]
    return [(lo * 128, (hi - lo) * 128) for lo, hi in zip(cuts, cuts[1:])]


def bit(me, axis):
    return lax.rem(me // axis, 2)


def flip(me, axis):
    return me + axis - 2 * axis * bit(me, axis)


def subsets(axes):
    sums = [0]
    for axis in axes:
        sums = sums + [s + axis for s in sums]
    return sums


def clear(me, axes):
    for axis in axes:
        me = me - axis * bit(me, axis)
    return me


def meet(me):
    barrier = pltpu.get_barrier_semaphore()
    for axis in (X, Y, Z, CORE):
        pl.semaphore_signal(barrier, inc=1, device_id={"dp": flip(me, axis)}, device_id_type=MESH)
    pl.semaphore_wait(barrier, 4)


class Sends:
    def __init__(self, send, recv):
        self.send, self.recv, self.used = send, recv, 0

    def start(self, source, target, to):
        n = self.used
        self.used += 1
        copy = pltpu.make_async_remote_copy(
            src_ref=source, dst_ref=target, send_sem=self.send.at[n], recv_sem=self.recv.at[n],
            device_id={"dp": to}, device_id_type=MESH,
        )
        copy.start()
        return copy


GATHER_COPIES = 3 * 7 + 8


def gather_kernel(layer, count, *refs):
    shards, fulls = refs[:count], refs[count : 2 * count]
    held, send, recv, local = refs[2 * count : 3 * count], *refs[3 * count :]
    me = lax.axis_index("dp")
    ins = [pltpu.make_async_copy(s.at[layer], h.at[me], local.at[m, 0]) for m, (s, h) in enumerate(zip(shards, held))]
    for copy in ins:
        copy.start()
    meet(me)
    sends = Sends(send, recv)
    flying = [[] for _ in range(count)]
    for stage in range(4):
        for m in range(count):
            if stage == 0:
                ins[m].wait()
            for copy in flying[m]:
                copy.wait()
            flying[m] = []
            if stage < 3:
                for (at, width), order in zip(thirds(held[m].shape[2]), ORDERS):
                    done, axis = order[:stage], order[stage]
                    for s in subsets(done):
                        block = held[m].at[clear(me, done) + s, :, pl.ds(at, width)]
                        flying[m].append(sends.start(block, block, flip(me, axis)))
            else:
                for s in subsets((X, Y, Z)):
                    block = held[m].at[clear(me, (X, Y, Z)) + s]
                    flying[m].append(sends.start(block, block, flip(me, CORE)))
    outs = []
    for m in range(count):
        for s in range(8):
            n = 2 * s + bit(me, CORE)
            outs.append(pltpu.make_async_copy(held[m].at[n], fulls[m].at[n], local.at[m, 1 + s]))
            outs[-1].start()
    for m in range(count):
        for s in range(8):
            flying[m][s].wait()
        for s in range(8):
            n = 2 * s + 1 - bit(me, CORE)
            outs.append(pltpu.make_async_copy(held[m].at[n], fulls[m].at[n], local.at[m, 9 + s]))
            outs[-1].start()
    for copy in outs:
        copy.wait()


def gather(shards, layer, collective_id):
    count = len(shards)
    shapes = [(16, *s.shape[1:]) for s in shards]
    fulls = pl.pallas_call(
        functools.partial(gather_kernel, layer, count),
        out_shape=[jax.ShapeDtypeStruct(s, bf16) for s in shapes],
        in_specs=[ANY] * count,
        out_specs=[ANY] * count,
        scratch_shapes=[pltpu.VMEM(s, bf16) for s in shapes]
        + [pltpu.SemaphoreType.DMA((count * GATHER_COPIES,))] * 2
        + [pltpu.SemaphoreType.DMA((count, 17))],
        compiler_params=pltpu.CompilerParams(collective_id=collective_id, has_side_effects=True, vmem_limit_bytes=60 * MIB),
        cost_estimate=pl.CostEstimate(flops=10 * 10**9 * count, bytes_accessed=10**7 * count, transcendentals=0),
        name="gather",
    )(*shards)
    return [t.reshape(-1, t.shape[2]) for t in fulls]


def scatter_kernel(count, *refs):
    terms, outs = refs[:count], refs[count : 2 * count]
    rest = refs[2 * count :]
    own, other, total, given, got = (rest[k * count : (k + 1) * count] for k in range(5))
    send, recv, local = rest[5 * count :]
    me = lax.axis_index("dp")
    core = bit(me, CORE)
    here = me // 2
    meet(me)
    sends = Sends(send, recv)
    flying, loads = [], []
    for m in range(count):
        flying.append([sends.start(terms[m].at[2 * j + 1 - core], other[m].at[j], flip(me, CORE)) for j in range(8)])
        loads.append([pltpu.make_async_copy(terms[m].at[2 * j + core], own[m].at[j], local.at[m, j]) for j in range(8)])
        for copy in loads[m]:
            copy.start()
    for stage in range(4):
        for m in range(count):
            for copy in flying[m]:
                copy.wait()
            flying[m] = []
            if stage == 0:
                for copy in loads[m]:
                    copy.wait()

                def add(j, _, m=m):
                    total[m][j] = own[m][j].astype(f32) + other[m][j].astype(f32)
                    return 0

                lax.fori_loop(0, 8, add, 0)
            base = (0, 0, 4, 6)[stage]
            cuts = list(zip(thirds(terms[m].shape[2]), ORDERS))
            if stage > 0:
                for (at, width), order in cuts:
                    left = [a // 2 for a in order[stage:]]
                    cols = pl.ds(at, width)
                    for k, s in enumerate(subsets(left)):
                        block = clear(here, left) + s
                        total[m][block, :, cols] = (
                            total[m][block, :, cols] + got[m][(0, 0, 4, 6)[stage] + k, :, cols].astype(f32)
                        )
            if stage < 3:
                base = (0, 4, 6)[stage]
                for (at, width), order in cuts:
                    axis, left = order[stage] // 2, [a // 2 for a in order[stage + 1 :]]
                    cols = pl.ds(at, width)
                    for k, s in enumerate(subsets(left)):
                        given[m][base + k, :, cols] = total[m][flip(clear(here, left), axis) + s, :, cols].astype(bf16)
                for (at, width), order in cuts:
                    cols = pl.ds(at, width)
                    for k in range((4, 2, 1)[stage]):
                        flying[m].append(
                            sends.start(
                                given[m].at[base + k, :, cols], got[m].at[base + k, :, cols], flip(me, order[stage])
                            )
                        )
            else:
                outs[m][...] = total[m][here].astype(bf16)


def scatter(terms, collective_id):
    count = len(terms)
    terms = [t.reshape(16, -1, t.shape[1]) for t in terms]
    blocks = [t.shape[1:] for t in terms]
    vmem = lambda n, dtype: [pltpu.VMEM((n, *b), dtype) for b in blocks]
    return pl.pallas_call(
        functools.partial(scatter_kernel, count),
        out_shape=[jax.ShapeDtypeStruct(b, bf16) for b in blocks],
        in_specs=[ANY] * count,
        out_specs=[pl.BlockSpec(memory_space=pltpu.VMEM)] * count,
        scratch_shapes=vmem(8, bf16) + vmem(8, bf16) + vmem(8, f32) + vmem(7, bf16) + vmem(7, bf16)
        + [pltpu.SemaphoreType.DMA((count * GATHER_COPIES,))] * 2
        + [pltpu.SemaphoreType.DMA((count, 8))],
        compiler_params=pltpu.CompilerParams(collective_id=collective_id, has_side_effects=True, vmem_limit_bytes=60 * MIB),
        cost_estimate=pl.CostEstimate(flops=10 * 10**9 * count, bytes_accessed=10**7 * count, transcendentals=0),
        name="scatter",
    )(*terms)


def dot(a, b, ca, cb):
    return lax.dot_general(a, b, (((ca,), (cb,)), ((), ())), preferred_element_type=f32)


def call(kernel, grid, ins, outs, args, matmuls, name):
    moved = sum(a.size * a.dtype.itemsize for a in args) + sum(
        functools.reduce(lambda p, q: p * q, s, 1) * jnp.dtype(d).itemsize for s, d, _, _ in outs
    )
    return pl.pallas_call(
        kernel,
        grid=grid,
        in_specs=[pl.BlockSpec(b, i) for b, i in ins],
        out_specs=[pl.BlockSpec(b, i) for _, _, b, i in outs],
        out_shape=[jax.ShapeDtypeStruct(s, d) for s, d, _, _ in outs],
        compiler_params=pltpu.CompilerParams(
            dimension_semantics=("arbitrary",) * len(grid), vmem_limit_bytes=56 * MIB
        ),
        cost_estimate=pl.CostEstimate(flops=matmuls * 2 * 2048 * 896 * 2560, bytes_accessed=moved, transcendentals=0),
        name=name,
    )(*args)


def scale_of(wide):
    return lax.rsqrt(jnp.mean(wide * wide, -1, keepdims=True) + 1e-6)


def normed(h):
    wide = h.astype(f32)
    return (wide * scale_of(wide)).astype(bf16)


def backward_of_product(by_p, gate, up):
    wide = by_p.astype(f32)
    sig = jax.nn.sigmoid(gate)
    swish = gate * sig
    by_up = wide * swish
    by_gate = wide * up * (sig + swish * (1 - sig))
    return by_gate.astype(bf16), by_up.astype(bf16)


def forward_kernel(a, wg, wu, gate, up, p):
    gate[...] = dot(a[...], wg[...], 1, 0)
    up[...] = dot(a[...], wu[...], 1, 0)
    g = gate[...]
    p[...] = (g * jax.nn.sigmoid(g) * up[...]).astype(bf16)


def turn_kernel(a, by_h, wg, wu, wd, p, by_gate, by_up):
    g = dot(a[...], wg[...], 1, 0)
    u = dot(a[...], wu[...], 1, 0)
    by_p = dot(by_h[...], wd[...], 1, 1).astype(bf16)
    p[...] = (g * jax.nn.sigmoid(g) * u).astype(bf16)
    by_gate[...], by_up[...] = backward_of_product(by_p, g, u)


def product_kernel(by_h, wd, gate, up, by_gate, by_up):
    by_p = dot(by_h[...], wd[...], 1, 1).astype(bf16)
    by_gate[...], by_up[...] = backward_of_product(by_p, gate[...], up[...])


def down_kernel(p, wd, x, h, a):
    out = x[...] + dot(p[...], wd[...], 1, 0).astype(bf16)
    h[...] = out
    a[...] = normed(out)


def input_kernel(by_gate, by_up, wg, wu, h, by_h, out):
    by_a = dot(by_gate[...], wg[...], 1, 1).astype(bf16) + dot(by_up[...], wu[...], 1, 1).astype(bf16)
    wide, ct = h[...].astype(f32), by_a.astype(f32)
    scale = scale_of(wide)
    by_mean = jnp.sum(ct * wide, -1, keepdims=True) * (-0.5 * scale * scale * scale)
    by_wide = ct * scale + by_mean * (2.0 / wide.shape[1]) * wide
    out[...] = by_h[...] + by_wide.astype(bf16)


def weight_kernel(left, right, out):
    out[...] = dot(left[...], right[...], 0, 0).astype(bf16)


def solution(mesh):
    def step(x, dy, w_gate, w_up, w_down):
        x, dy = x[0], dy[0]
        t, d = x.shape
        ff = w_gate.shape[2]
        bn, bm, bh = 512, 1024, 512

        def whole(w):
            return lax.all_gather(w, "dp", axis=0, tiled=True)

        rows = lambda width: ((bm, width), lambda j, i: (i, 0))
        cols = ((d, bn), lambda j, i: (0, j))
        down = ((bn, d), lambda j, i: (j, 0))
        tile = ((bm, bn), lambda j, i: (i, j))
        slab = lambda width: ((bh, width), lambda i: (i, 0))
        full = lambda a: (a.shape, lambda i: (0, 0))
        both = (ff // bn, t // bm)

        def weight(left, right, name):
            m, n = left.shape[1], right.shape[1]
            if n > m:
                ins, out = [full(left), ((t, bn), lambda j: (0, j))], ((m, bn), lambda j: (0, j))
            else:
                ins, out = [((t, bn), lambda j: (0, j)), full(right)], ((bn, n), lambda j: (j, 0))
            return call(weight_kernel, (ff // bn,), ins, [((m, n), bf16, *out)], (left, right), 1, name)[0]

        def to_input(by_gate, by_up, wg, wu, h, by_h):
            ins = [slab(ff), slab(ff), full(wg), full(wu), slab(d), slab(d)]
            outs = [((t, d), bf16, *slab(d))]
            return call(input_kernel, (t // bh,), ins, outs, (by_gate, by_up, wg, wu, h, by_h), 2, "to_input")[0]

        wg0, wu0 = gather((w_gate, w_up), 0, 0)
        wd0, wg1, wu1, wd1 = whole(w_down[0]), whole(w_gate[1]), whole(w_up[1]), whole(w_down[1])

        a0 = normed(x)
        gate0, up0, p0 = call(
            forward_kernel, both, [rows(d), cols, cols],
            [((t, ff), f32, *tile), ((t, ff), f32, *tile), ((t, ff), bf16, *tile)], (a0, wg0, wu0), 2, "forward",
        )
        h1, a1 = call(
            down_kernel, (t // bh,), [slab(ff), full(wd0), slab(d)], [((t, d), bf16, *slab(d))] * 2, (p0, wd0, x), 1, "down"
        )
        p1, by_gate1, by_up1 = call(
            turn_kernel, both, [rows(d), rows(d), cols, cols, down], [((t, ff), bf16, *tile)] * 3,
            (a1, dy, wg1, wu1, wd1), 3, "turn",
        )
        terms1 = [weight(a1, by_gate1, "g_gate"), weight(a1, by_up1, "g_up"), weight(p1, dy, "g_down")]
        by_gate1, by_up1, *_ = lax.optimization_barrier((by_gate1, by_up1, *terms1))
        grads1 = [lax.psum_scatter(g, "dp", scatter_dimension=0, tiled=True) for g in terms1]
        by_h1 = to_input(by_gate1, by_up1, wg1, wu1, h1, dy)
        by_gate0, by_up0 = call(
            product_kernel, both, [rows(d), down, tile, tile], [((t, ff), bf16, *tile)] * 2, (by_h1, wd0, gate0, up0), 1,
            "product",
        )
        terms0 = [weight(a0, by_gate0, "g_gate"), weight(a0, by_up0, "g_up"), weight(p0, by_h1, "g_down")]
        grads0 = scatter(terms0, 1)
        by_x = to_input(by_gate0, by_up0, wg0, wu0, x, by_h1)
        return (by_x[None], *(jnp.stack([g0, g1]) for g0, g1 in zip(grads0, grads1)))

    tok = P(("rep", "dp"), None, None)
    w = P(None, "dp", None)
    g = P("rep", "dp", None)
    return jax.shard_map(step, mesh=mesh, in_specs=(tok, tok, w, w, w), out_specs=(tok, g, g, g), check_vma=False)
```

```python
import functools

import jax
import jax.numpy as jnp
from jax import lax
from jax.experimental import pallas as pl
from jax.experimental.pallas import tpu as pltpu
from jax.sharding import PartitionSpec as P

bf16, f32 = jnp.bfloat16, jnp.float32
MESH = pl.DeviceIdType.MESH
ANY = pl.BlockSpec(memory_space=pl.ANY)
MIB = 1 << 20
CORE, Z, Y, X = 1, 2, 4, 8
ORDERS = ((X, Y, Z), (Y, Z, X), (Z, X, Y))


def thirds(columns):
    tiles = columns // 128
    cuts = [0, (tiles + 2) // 3, (tiles + 2) // 3 + (tiles + 1) // 3, tiles]
    return [(lo * 128, (hi - lo) * 128) for lo, hi in zip(cuts, cuts[1:])]


def bit(me, axis):
    return lax.rem(me // axis, 2)


def flip(me, axis):
    return me + axis - 2 * axis * bit(me, axis)


def subsets(axes):
    sums = [0]
    for axis in axes:
        sums = sums + [s + axis for s in sums]
    return sums


def chosen(axes, k):
    return sum(axis * lax.rem(k // 2**i, 2) for i, axis in enumerate(axes))


def clear(me, axes):
    for axis in axes:
        me = me - axis * bit(me, axis)
    return me


def meet(me):
    barrier = pltpu.get_barrier_semaphore()
    for axis in (X, Y, Z, CORE):
        pl.semaphore_signal(barrier, inc=1, device_id={"dp": flip(me, axis)}, device_id_type=MESH)
    pl.semaphore_wait(barrier, 4)


class Gather:
    def __init__(self, shards, layer):
        self.args, self.layer, self.count = list(shards), layer, len(shards)
        shapes = [(16, *s.shape[1:]) for s in shards]
        self.in_specs = [ANY] * self.count
        self.outs = [jax.ShapeDtypeStruct(s, bf16) for s in shapes]
        self.out_specs = [ANY] * self.count
        self.scratch = [pltpu.VMEM(s, bf16) for s in shapes] + [
            pltpu.SemaphoreType.DMA((self.count * COPIES,)),
            pltpu.SemaphoreType.DMA((self.count * COPIES,)),
            pltpu.SemaphoreType.DMA((self.count, 17)),
        ]

    def bind(self, shards, fulls, scratch):
        count = self.count
        held, (send, recv, local) = scratch[:count], scratch[count:]
        me = lax.axis_index("dp")

        def ins(m):
            return pltpu.make_async_copy(shards[m].at[self.layer], held[m].at[me], local.at[m, 0])

        def sends(m, stage):
            n = m * COPIES + (0, 3, 9, 21)[stage]
            found = []
            if stage == 3:
                for k, s in enumerate(subsets((X, Y, Z))):
                    block = held[m].at[clear(me, (X, Y, Z)) + s]
                    found.append(remote(block, block, send.at[n + k], recv.at[n + k], flip(me, CORE)))
                return found
            for (at, width), order in zip(thirds(held[m].shape[2]), ORDERS):
                for s in subsets(order[:stage]):
                    block = held[m].at[clear(me, order[:stage]) + s, :, pl.ds(at, width)]
                    k = n + len(found)
                    found.append(remote(block, block, send.at[k], recv.at[k], flip(me, order[stage])))
            return found

        def outs(m, core, at):
            return [
                pltpu.make_async_copy(held[m].at[2 * s + core], fulls[m].at[2 * s + core], local.at[m, at + s])
                for s in range(8)
            ]

        def phase(stage):
            def run():
                if stage == 0:
                    for m in range(count):
                        ins(m).start()
                    meet(me)
                for m in range(count):
                    if stage == 0:
                        ins(m).wait()
                    else:
                        for copy in sends(m, stage - 1):
                            copy.wait()
                    if stage < 4:
                        for copy in sends(m, stage):
                            copy.start()
                    if stage == 3:
                        for copy in outs(m, bit(me, CORE), 1):
                            copy.start()
                    if stage == 4:
                        for copy in outs(m, 1 - bit(me, CORE), 9):
                            copy.start()
                if stage == 4:
                    for m in range(count):
                        for copy in outs(m, bit(me, CORE), 1) + outs(m, 1 - bit(me, CORE), 9):
                            copy.wait()

            return run

        return [phase(stage) for stage in range(5)]


class Scatter:
    def __init__(self, terms):
        self.args = [t.reshape(16, -1, t.shape[1]) for t in terms]
        self.count = len(terms)
        blocks = [t.shape[1:] for t in self.args]
        self.in_specs = [ANY] * self.count
        self.outs = [jax.ShapeDtypeStruct(b, bf16) for b in blocks]
        self.out_specs = [pl.BlockSpec(b, lambda *_: (0, 0)) for b in blocks]
        vmem = lambda n, dtype: [pltpu.VMEM((n, *b), dtype) for b in blocks]
        self.scratch = vmem(8, bf16) + vmem(8, f32) + vmem(8, bf16) + vmem(7, bf16) + [
            pltpu.SemaphoreType.DMA((self.count * COPIES,)),
            pltpu.SemaphoreType.DMA((self.count * COPIES,)),
            pltpu.SemaphoreType.DMA((self.count, 8)),
        ]

    def bind(self, terms, results, scratch):
        count = self.count
        other, total, given, got = (scratch[k * count : (k + 1) * count] for k in range(4))
        send, recv, local = scratch[4 * count :]
        me = lax.axis_index("dp")
        core, here = bit(me, CORE), me // 2

        def loads(m):
            return [pltpu.make_async_copy(terms[m].at[2 * j + core], given[m].at[j], local.at[m, j]) for j in range(8)]

        def sends(m, stage):
            n = m * COPIES + (0, 8, 20, 26)[stage]
            if stage == 0:
                return [
                    remote(terms[m].at[2 * j + 1 - core], other[m].at[j], send.at[n + j], recv.at[n + j], flip(me, CORE))
                    for j in range(8)
                ]
            base, found = (0, 0, 4, 6)[stage], []
            for (at, width), order in zip(thirds(terms[m].shape[2]), ORDERS):
                for k in range((0, 4, 2, 1)[stage]):
                    part = (base + k, slice(None), pl.ds(at, width))
                    i = n + len(found)
                    found.append(remote(given[m].at[part], got[m].at[part], send.at[i], recv.at[i], flip(me, order[stage - 1])))
            return found

        def phase(stage):
            def run():
                if stage == 0:
                    meet(me)
                    for m in range(count):
                        for copy in sends(m, 0) + loads(m):
                            copy.start()
                    return
                for m in range(count):
                    for copy in sends(m, stage - 1):
                        copy.wait()
                    cuts = list(zip(thirds(terms[m].shape[2]), ORDERS))
                    if stage == 1:
                        for copy in loads(m):
                            copy.wait()

                        def add(j, _, m=m):
                            total[m][j] = given[m][j].astype(f32) + other[m][j].astype(f32)
                            return 0

                        lax.fori_loop(0, 8, add, 0)
                    else:
                        for (at, width), order in cuts:
                            left = [axis // 2 for axis in order[stage - 1 :]]
                            cols = pl.ds(at, width)

                            def take(k, _, m=m, left=left, cols=cols):
                                block = clear(here, left) + chosen(left, k)
                                arrived = got[m][(0, 0, 0, 4, 6)[stage] + k, :, cols].astype(f32)
                                total[m][block, :, cols] = total[m][block, :, cols] + arrived
                                return 0

                            lax.fori_loop(0, 2 ** len(left), take, 0)
                    if stage == 4:
                        results[m][...] = total[m][here].astype(bf16)
                        continue
                    base = (0, 0, 4, 6)[stage]
                    for (at, width), order in cuts:
                        axis, left = order[stage - 1] // 2, [a // 2 for a in order[stage:]]
                        cols = pl.ds(at, width)

                        def give(k, _, m=m, axis=axis, left=left, cols=cols):
                            block = flip(clear(here, left), axis) + chosen(left, k)
                            given[m][base + k, :, cols] = total[m][block, :, cols].astype(bf16)
                            return 0

                        lax.fori_loop(0, 2 ** len(left), give, 0)
                    for copy in sends(m, stage):
                        copy.start()

            return run

        return [phase(stage) for stage in range(5)]


def remote(source, target, send, recv, to):
    return pltpu.make_async_remote_copy(
        src_ref=source, dst_ref=target, send_sem=send, recv_sem=recv, device_id={"dp": to}, device_id_type=MESH
    )


COPIES = 3 * 7 + 8


def dot(a, b, ca, cb):
    return lax.dot_general(a, b, (((ca,), (cb,)), ((), ())), preferred_element_type=f32)


def call(kernel, grid, ins, outs, args, matmuls, name, comm=None, steps=(), collective_id=None):
    args, n_in, n_out = list(args), len(args), len(outs)
    moved = sum(a.size * a.dtype.itemsize for a in args) + sum(
        functools.reduce(lambda p, q: p * q, s, 1) * jnp.dtype(d).itemsize for s, d, _, _ in outs
    )
    in_specs = [
        pl.BlockSpec(b, i, pipeline_mode=pl.Buffered(1)) if tuple(b) == a.shape else pl.BlockSpec(b, i)
        for a, (b, i) in zip(args, ins)
    ]
    out_specs = [pl.BlockSpec(b, i) for _, _, b, i in outs]
    out_shape = [jax.ShapeDtypeStruct(s, d) for s, d, _, _ in outs]
    params = dict(dimension_semantics=("arbitrary",) * len(grid), vmem_limit_bytes=58 * MIB)
    body, scratch = kernel, []
    if comm is not None:
        in_specs, out_specs, out_shape = in_specs + comm.in_specs, out_specs + comm.out_specs, out_shape + comm.outs
        args, scratch = args + comm.args, comm.scratch
        params.update(collective_id=collective_id, has_side_effects=True, vmem_limit_bytes=63 * MIB)

        def body(*refs):
            mine, refs = refs[:n_in], refs[n_in:]
            theirs, refs = refs[: comm.count], refs[comm.count :]
            made, refs = refs[:n_out], refs[n_out:]
            phases = comm.bind(theirs, refs[: comm.count], refs[comm.count :])
            step = pl.program_id(0)
            for axis in range(1, len(grid)):
                step = step * grid[axis] + pl.program_id(axis)
            for at, phase in zip(steps, phases):
                if at >= 0:
                    pl.when(step == at)(phase)
            if n_in:
                kernel(*mine, *made)
            for at, phase in zip(steps, phases):
                if at < 0:
                    pl.when(step == -1 - at)(phase)

    return pl.pallas_call(
        body,
        grid=grid,
        in_specs=in_specs,
        out_specs=out_specs,
        out_shape=out_shape,
        scratch_shapes=scratch,
        compiler_params=pltpu.CompilerParams(**params),
        cost_estimate=pl.CostEstimate(
            flops=max(matmuls, 1) * 2 * 2048 * 896 * 2560, bytes_accessed=max(moved, 10**7), transcendentals=0
        ),
        name=name,
    )(*args)


def scale_of(wide):
    return lax.rsqrt(jnp.mean(wide * wide, -1, keepdims=True) + 1e-6)


def normed(h):
    wide = h.astype(f32)
    return (wide * scale_of(wide)).astype(bf16)


def halves(width):
    return [pl.ds(at, 256) for at in range(0, width, 256)]


def forward_kernel(a, wg, wu, swish, slope, p):
    for cols in halves(p.shape[1]):
        g = dot(a[...], wg[:, cols], 1, 0)
        u = dot(a[...], wu[:, cols], 1, 0)
        sig = jax.nn.sigmoid(g)
        s = g * sig
        swish[:, cols] = s
        slope[:, cols] = (0.5 * u) * (sig + s * (1 - sig))
        p[:, cols] = (s * u).astype(bf16)


def turn_kernel(a, by_h, wg, wu, wd, p, by_gate, by_up):
    for cols in halves(p.shape[1]):
        g = dot(a[...], wg[:, cols], 1, 0)
        u = dot(a[...], wu[:, cols], 1, 0)
        by_p = dot(by_h[...], wd[cols, :], 1, 1).astype(bf16).astype(f32)
        sig = jax.nn.sigmoid(g)
        s = g * sig
        p[:, cols] = (s * u).astype(bf16)
        by_up[:, cols] = (by_p * s).astype(bf16)
        by_gate[:, cols] = (by_p * u * (sig + s * (1 - sig))).astype(bf16)


def product_kernel(by_h, wd, swish, slope, by_gate, by_up):
    for cols in halves(by_up.shape[1]):
        by_p = dot(by_h[...], wd[cols, :], 1, 1).astype(bf16).astype(f32)
        by_up[:, cols] = (by_p * swish[:, cols]).astype(bf16)
        by_gate[:, cols] = (by_p * slope[:, cols] * 2).astype(bf16)


def down_kernel(p, wd, x, h, a):
    out = x[...] + dot(p[...], wd[...], 1, 0).astype(bf16)
    h[...] = out
    a[...] = normed(out)


def input_kernel(by_gate, by_up, wg, wu, h, by_h, out):
    by_a = dot(by_gate[...], wg[...], 1, 1).astype(bf16) + dot(by_up[...], wu[...], 1, 1).astype(bf16)
    wide, ct = h[...].astype(f32), by_a.astype(f32)
    scale = scale_of(wide)
    by_mean = jnp.sum(ct * wide, -1, keepdims=True) * (-0.5 * scale * scale * scale)
    by_wide = ct * scale + by_mean * (2.0 / wide.shape[1]) * wide
    out[...] = by_h[...] + by_wide.astype(bf16)


def weight_kernel(left, right, out):
    out[...] = dot(left[...], right[...], 0, 0).astype(bf16)


def solution(mesh):
    def step(x, dy, w_gate, w_up, w_down):
        x, dy = x[0], dy[0]
        t, d = x.shape
        ff = w_gate.shape[2]
        bn, bm, bh = 512, 1024, 512

        def whole(w):
            return lax.all_gather(w, "dp", axis=0, tiled=True)

        rows = lambda width: ((bm, width), lambda j, i: (i, 0))
        cols = ((d, bn), lambda j, i: (0, j))
        down = ((bn, d), lambda j, i: (j, 0))
        tile = ((bm, bn), lambda j, i: (i, j))
        slab = lambda width: ((bh, width), lambda i: (i, 0))
        full = lambda a: (a.shape, lambda i: (0, 0))
        both = (ff // bn, t // bm)

        def weight(left, right, name):
            m, n = left.shape[1], right.shape[1]
            if n > m:
                ins, out = [full(left), ((t, bn), lambda j: (0, j))], ((m, bn), lambda j: (0, j))
            else:
                ins, out = [((t, bn), lambda j: (0, j)), full(right)], ((bn, n), lambda j: (j, 0))
            return call(weight_kernel, (ff // bn,), ins, [((m, n), bf16, *out)], (left, right), 1, name)[0]

        def to_input(by_gate, by_up, wg, wu, h, by_h, comm, steps, collective_id):
            ins = [slab(ff), slab(ff), full(wg), full(wu), slab(d), slab(d)]
            outs = [((t, d), bf16, *slab(d))]
            args = (by_gate, by_up, wg, wu, h, by_h)
            return call(input_kernel, (t // bh,), ins, outs, args, 2, "to_input", comm, steps, collective_id)

        matrix = lambda t: t.reshape(-1, t.shape[2])
        wg0, wu0 = map(matrix, call(None, (1,), [], [], (), 2, "gather", Gather((w_gate, w_up), 0), (0,) * 5, 0))
        wd0, wd1 = whole(w_down[0]), whole(w_down[1])

        a0 = normed(x)
        swish0, slope0, p0, wg1, wu1 = call(
            forward_kernel, both, [rows(d), cols, cols],
            [((t, ff), f32, *tile), ((t, ff), f32, *tile), ((t, ff), bf16, *tile)], (a0, wg0, wu0), 2, "forward",
            Gather((w_gate, w_up), 1), (0, 1, 3, 7, -10), 1,
        )
        wg1, wu1 = matrix(wg1), matrix(wu1)
        h1, a1 = call(
            down_kernel, (t // bh,), [slab(ff), full(wd0), slab(d)], [((t, d), bf16, *slab(d))] * 2, (p0, wd0, x), 1, "down"
        )
        p1, by_gate1, by_up1 = call(
            turn_kernel, both, [rows(d), rows(d), cols, cols, down], [((t, ff), bf16, *tile)] * 3,
            (a1, dy, wg1, wu1, wd1), 3, "turn",
        )
        g_gate1, g_up1 = weight(a1, by_gate1, "g_gate"), weight(a1, by_up1, "g_up")
        p1, _ = lax.optimization_barrier((p1, g_up1))
        g_down1 = weight(p1, dy, "g_down")
        g_gate1, g_up1 = (lax.psum_scatter(g, "dp", scatter_dimension=0, tiled=True) for g in (g_gate1, g_up1))
        by_h1, g_down1 = to_input(by_gate1, by_up1, wg1, wu1, h1, dy, Scatter((g_down1,)), (0, 1, 2, 3, -4), 2)
        g_down0 = weight(p0, by_h1, "g_down")
        by_gate0, by_up0, g_down0 = call(
            product_kernel, both, [rows(d), down, tile, tile], [((t, ff), bf16, *tile)] * 2, (by_h1, wd0, swish0, slope0), 1,
            "product", Scatter((g_down0,)), (0, 2, 5, 7, -10), 3,
        )
        terms0 = [weight(a0, by_gate0, "g_gate"), weight(a0, by_up0, "g_up")]
        by_x, g_gate0, g_up0 = to_input(by_gate0, by_up0, wg0, wu0, x, by_h1, Scatter(terms0), (0, 1, 3, -4, -4), 4)
        grads0, grads1 = (g_gate0, g_up0, g_down0), (g_gate1, g_up1, g_down1)
        return (by_x[None], *(jnp.stack([g0, g1]) for g0, g1 in zip(grads0, grads1)))

    tok = P(("rep", "dp"), None, None)
    w = P(None, "dp", None)
    g = P("rep", "dp", None)
    return jax.shard_map(step, mesh=mesh, in_specs=(tok, tok, w, w, w), out_specs=(tok, g, g, g), check_vma=False)
```

```python
import functools

import jax
import jax.numpy as jnp
from jax import lax
from jax.experimental import pallas as pl
from jax.experimental.pallas import tpu as pltpu
from jax.sharding import PartitionSpec as P

bf16, f32 = jnp.bfloat16, jnp.float32
MESH = pl.DeviceIdType.MESH
ANY = pl.BlockSpec(memory_space=pl.ANY)
MIB = 1 << 20
CORE, Z, Y, X = 1, 2, 4, 8
ORDERS = ((X, Y, Z), (Y, Z, X), (Z, X, Y))


def thirds(columns):
    tiles = columns // 128
    cuts = [0, (tiles + 2) // 3, (tiles + 2) // 3 + (tiles + 1) // 3, tiles]
    return [(lo * 128, (hi - lo) * 128) for lo, hi in zip(cuts, cuts[1:])]


def bit(me, axis):
    return lax.rem(me // axis, 2)


def flip(me, axis):
    return me + axis - 2 * axis * bit(me, axis)


def subsets(axes):
    sums = [0]
    for axis in axes:
        sums = sums + [s + axis for s in sums]
    return sums


def chosen(axes, k):
    return sum(axis * lax.rem(k // 2**i, 2) for i, axis in enumerate(axes))


def clear(me, axes):
    for axis in axes:
        me = me - axis * bit(me, axis)
    return me


def meet(me):
    barrier = pltpu.get_barrier_semaphore()
    for axis in (X, Y, Z, CORE):
        pl.semaphore_signal(barrier, inc=1, device_id={"dp": flip(me, axis)}, device_id_type=MESH)
    pl.semaphore_wait(barrier, 4)


class Gather:
    def __init__(self, shards, layers):
        self.args, self.layers, self.count = list(shards), layers, len(shards)
        shapes = [(16, *s.shape[1:]) for s in shards]
        self.in_specs = [ANY] * self.count
        self.outs = [jax.ShapeDtypeStruct(s, bf16) for s in shapes]
        self.out_specs = [ANY] * self.count
        self.scratch = [pltpu.VMEM(s, bf16) for s in shapes] + [
            pltpu.SemaphoreType.DMA((self.count * COPIES,)),
            pltpu.SemaphoreType.DMA((self.count * COPIES,)),
            pltpu.SemaphoreType.DMA((self.count, 17)),
        ]

    def bind(self, shards, fulls, scratch):
        count = self.count
        held, (send, recv, local) = scratch[:count], scratch[count:]
        me = lax.axis_index("dp")

        def ins(m):
            return pltpu.make_async_copy(shards[m].at[self.layers[m]], held[m].at[me], local.at[m, 0])

        def sends(m, stage):
            n = m * COPIES + (0, 3, 9, 21)[stage]
            found = []
            if stage == 3:
                for k, s in enumerate(subsets((X, Y, Z))):
                    block = held[m].at[clear(me, (X, Y, Z)) + s]
                    found.append(remote(block, block, send.at[n + k], recv.at[n + k], flip(me, CORE)))
                return found
            for (at, width), order in zip(thirds(held[m].shape[2]), ORDERS):
                for s in subsets(order[:stage]):
                    block = held[m].at[clear(me, order[:stage]) + s, :, pl.ds(at, width)]
                    k = n + len(found)
                    found.append(remote(block, block, send.at[k], recv.at[k], flip(me, order[stage])))
            return found

        def outs(m, core, at):
            return [
                pltpu.make_async_copy(held[m].at[2 * s + core], fulls[m].at[2 * s + core], local.at[m, at + s])
                for s in range(8)
            ]

        def phase(stage):
            def run():
                if stage == 0:
                    for m in range(count):
                        ins(m).start()
                    meet(me)
                for m in range(count):
                    if stage == 0:
                        ins(m).wait()
                    else:
                        for copy in sends(m, stage - 1):
                            copy.wait()
                    if stage < 4:
                        for copy in sends(m, stage):
                            copy.start()
                    if stage == 3:
                        for copy in outs(m, bit(me, CORE), 1):
                            copy.start()
                    if stage == 4:
                        for copy in outs(m, 1 - bit(me, CORE), 9):
                            copy.start()
                if stage == 4:
                    for m in range(count):
                        for copy in outs(m, bit(me, CORE), 1) + outs(m, 1 - bit(me, CORE), 9):
                            copy.wait()

            return run

        return [phase(stage) for stage in range(5)]


class Scatter:
    def __init__(self, terms):
        self.args = [t.reshape(16, -1, t.shape[1]) for t in terms]
        self.count = len(terms)
        blocks = [t.shape[1:] for t in self.args]
        self.in_specs = [ANY] * self.count
        self.outs = [jax.ShapeDtypeStruct(b, bf16) for b in blocks]
        self.out_specs = [pl.BlockSpec(b, lambda *_: (0, 0)) for b in blocks]
        vmem = lambda n, dtype: [pltpu.VMEM((n, *b), dtype) for b in blocks]
        self.scratch = vmem(8, bf16) + vmem(8, f32) + vmem(8, bf16) + vmem(7, bf16) + [
            pltpu.SemaphoreType.DMA((self.count * COPIES,)),
            pltpu.SemaphoreType.DMA((self.count * COPIES,)),
            pltpu.SemaphoreType.DMA((self.count, 8)),
        ]

    def bind(self, terms, results, scratch):
        count = self.count
        other, total, given, got = (scratch[k * count : (k + 1) * count] for k in range(4))
        send, recv, local = scratch[4 * count :]
        me = lax.axis_index("dp")
        core, here = bit(me, CORE), me // 2

        def loads(m):
            return [pltpu.make_async_copy(terms[m].at[2 * j + core], given[m].at[j], local.at[m, j]) for j in range(8)]

        def sends(m, stage):
            n = m * COPIES + (0, 8, 20, 26)[stage]
            if stage == 0:
                return [
                    remote(terms[m].at[2 * j + 1 - core], other[m].at[j], send.at[n + j], recv.at[n + j], flip(me, CORE))
                    for j in range(8)
                ]
            base, found = (0, 0, 4, 6)[stage], []
            for (at, width), order in zip(thirds(terms[m].shape[2]), ORDERS):
                for k in range((0, 4, 2, 1)[stage]):
                    part = (base + k, slice(None), pl.ds(at, width))
                    i = n + len(found)
                    found.append(remote(given[m].at[part], got[m].at[part], send.at[i], recv.at[i], flip(me, order[stage - 1])))
            return found

        def phase(stage):
            def run():
                if stage == 0:
                    meet(me)
                    for m in range(count):
                        for copy in sends(m, 0) + loads(m):
                            copy.start()
                    return
                for m in range(count):
                    for copy in sends(m, stage - 1):
                        copy.wait()
                    cuts = list(zip(thirds(terms[m].shape[2]), ORDERS))
                    if stage == 1:
                        for copy in loads(m):
                            copy.wait()

                        def add(j, _, m=m):
                            total[m][j] = given[m][j].astype(f32) + other[m][j].astype(f32)
                            return 0

                        lax.fori_loop(0, 8, add, 0)
                    else:
                        for (at, width), order in cuts:
                            left = [axis // 2 for axis in order[stage - 1 :]]
                            cols = pl.ds(at, width)

                            def take(k, _, m=m, left=left, cols=cols):
                                block = clear(here, left) + chosen(left, k)
                                arrived = got[m][(0, 0, 0, 4, 6)[stage] + k, :, cols].astype(f32)
                                total[m][block, :, cols] = total[m][block, :, cols] + arrived
                                return 0

                            lax.fori_loop(0, 2 ** len(left), take, 0)
                    if stage == 4:
                        results[m][...] = total[m][here].astype(bf16)
                        continue
                    base = (0, 0, 4, 6)[stage]
                    for (at, width), order in cuts:
                        axis, left = order[stage - 1] // 2, [a // 2 for a in order[stage:]]
                        cols = pl.ds(at, width)

                        def give(k, _, m=m, axis=axis, left=left, cols=cols):
                            block = flip(clear(here, left), axis) + chosen(left, k)
                            given[m][base + k, :, cols] = total[m][block, :, cols].astype(bf16)
                            return 0

                        lax.fori_loop(0, 2 ** len(left), give, 0)
                    for copy in sends(m, stage):
                        copy.start()

            return run

        return [phase(stage) for stage in range(5)]


def remote(source, target, send, recv, to):
    return pltpu.make_async_remote_copy(
        src_ref=source, dst_ref=target, send_sem=send, recv_sem=recv, device_id={"dp": to}, device_id_type=MESH
    )


COPIES = 3 * 7 + 8


def dot(a, b, ca, cb):
    return lax.dot_general(a, b, (((ca,), (cb,)), ((), ())), preferred_element_type=f32)


def call(kernel, grid, ins, outs, args, matmuls, name, comm=None, steps=(), collective_id=None):
    args, n_in, n_out = list(args), len(args), len(outs)
    moved = sum(a.size * a.dtype.itemsize for a in args) + sum(
        functools.reduce(lambda p, q: p * q, s, 1) * jnp.dtype(d).itemsize for s, d, _, _ in outs
    )
    in_specs = [
        pl.BlockSpec(b, i, pipeline_mode=pl.Buffered(1)) if tuple(b) == a.shape else pl.BlockSpec(b, i)
        for a, (b, i) in zip(args, ins)
    ]
    out_specs = [pl.BlockSpec(b, i) for _, _, b, i in outs]
    out_shape = [jax.ShapeDtypeStruct(s, d) for s, d, _, _ in outs]
    params = dict(dimension_semantics=("arbitrary",) * len(grid), vmem_limit_bytes=58 * MIB)
    body, scratch = kernel, []
    if comm is not None:
        in_specs, out_specs, out_shape = in_specs + comm.in_specs, out_specs + comm.out_specs, out_shape + comm.outs
        args, scratch = args + comm.args, comm.scratch
        params.update(collective_id=collective_id, has_side_effects=True, vmem_limit_bytes=63 * MIB)

        def body(*refs):
            mine, refs = refs[:n_in], refs[n_in:]
            theirs, refs = refs[: comm.count], refs[comm.count :]
            made, refs = refs[:n_out], refs[n_out:]
            phases = comm.bind(theirs, refs[: comm.count], refs[comm.count :])
            step = pl.program_id(0)
            for axis in range(1, len(grid)):
                step = step * grid[axis] + pl.program_id(axis)
            for at, phase in zip(steps, phases):
                if at >= 0:
                    pl.when(step == at)(phase)
            if n_in:
                kernel(*mine, *made)
            for at, phase in zip(steps, phases):
                if at < 0:
                    pl.when(step == -1 - at)(phase)

    return pl.pallas_call(
        body,
        grid=grid,
        in_specs=in_specs,
        out_specs=out_specs,
        out_shape=out_shape,
        scratch_shapes=scratch,
        compiler_params=pltpu.CompilerParams(**params),
        cost_estimate=pl.CostEstimate(
            flops=max(matmuls, 1) * 2 * 2048 * 896 * 2560, bytes_accessed=max(moved, 10**7), transcendentals=0
        ),
        name=name,
    )(*args)


def scale_of(wide):
    return lax.rsqrt(jnp.mean(wide * wide, -1, keepdims=True) + 1e-6)


def normed(h):
    wide = h.astype(f32)
    return (wide * scale_of(wide)).astype(bf16)


def halves(width):
    return [pl.ds(at, 256) for at in range(0, width, 256)]


def forward_kernel(a, wg, wu, swish, slope, p):
    for cols in halves(p.shape[1]):
        g = dot(a[...], wg[:, cols], 1, 0)
        u = dot(a[...], wu[:, cols], 1, 0)
        sig = jax.nn.sigmoid(g)
        s = g * sig
        swish[:, cols] = s
        slope[:, cols] = (0.5 * u) * (sig + s * (1 - sig))
        p[:, cols] = (s * u).astype(bf16)


def turn_kernel(a, by_h, wg, wu, wd, p, by_gate, by_up):
    for cols in halves(p.shape[1]):
        g = dot(a[...], wg[:, cols], 1, 0)
        u = dot(a[...], wu[:, cols], 1, 0)
        by_p = dot(by_h[...], wd[cols, :], 1, 1).astype(bf16).astype(f32)
        sig = jax.nn.sigmoid(g)
        s = g * sig
        p[:, cols] = (s * u).astype(bf16)
        by_up[:, cols] = (by_p * s).astype(bf16)
        by_gate[:, cols] = (by_p * u * (sig + s * (1 - sig))).astype(bf16)


def product_kernel(by_h, wd, swish, slope, by_gate, by_up):
    for cols in halves(by_up.shape[1]):
        by_p = dot(by_h[...], wd[cols, :], 1, 1).astype(bf16).astype(f32)
        by_up[:, cols] = (by_p * swish[:, cols]).astype(bf16)
        by_gate[:, cols] = (by_p * slope[:, cols] * 2).astype(bf16)


def down_kernel(p, wd, x, h, a):
    out = x[...] + dot(p[...], wd[...], 1, 0).astype(bf16)
    h[...] = out
    a[...] = normed(out)


def input_kernel(by_gate, by_up, wg, wu, h, by_h, out):
    by_a = dot(by_gate[...], wg[...], 1, 1).astype(bf16) + dot(by_up[...], wu[...], 1, 1).astype(bf16)
    wide, ct = h[...].astype(f32), by_a.astype(f32)
    scale = scale_of(wide)
    by_mean = jnp.sum(ct * wide, -1, keepdims=True) * (-0.5 * scale * scale * scale)
    by_wide = ct * scale + by_mean * (2.0 / wide.shape[1]) * wide
    out[...] = by_h[...] + by_wide.astype(bf16)


def weight_kernel(left, right, out):
    out[...] = dot(left[...], right[...], 0, 0).astype(bf16)


def solution(mesh):
    def step(x, dy, w_gate, w_up, w_down):
        x, dy = x[0], dy[0]
        t, d = x.shape
        ff = w_gate.shape[2]
        bn, bm, bh = 512, 1024, 512

        def whole(w):
            return lax.all_gather(w, "dp", axis=0, tiled=True)

        rows = lambda width: ((bm, width), lambda j, i: (i, 0))
        cols = ((d, bn), lambda j, i: (0, j))
        down = ((bn, d), lambda j, i: (j, 0))
        tile = ((bm, bn), lambda j, i: (i, j))
        slab = lambda width: ((bh, width), lambda i: (i, 0))
        full = lambda a: (a.shape, lambda i: (0, 0))
        both = (ff // bn, t // bm)

        def weight(left, right, name):
            m, n = left.shape[1], right.shape[1]
            if n > m:
                ins, out = [full(left), ((t, bn), lambda j: (0, j))], ((m, bn), lambda j: (0, j))
            else:
                ins, out = [((t, bn), lambda j: (0, j)), full(right)], ((bn, n), lambda j: (j, 0))
            return call(weight_kernel, (ff // bn,), ins, [((m, n), bf16, *out)], (left, right), 1, name)[0]

        def to_input(by_gate, by_up, wg, wu, h, by_h, comm, steps, collective_id):
            ins = [slab(ff), slab(ff), full(wg), full(wu), slab(d), slab(d)]
            outs = [((t, d), bf16, *slab(d))]
            args = (by_gate, by_up, wg, wu, h, by_h)
            return call(input_kernel, (t // bh,), ins, outs, args, 2, "to_input", comm, steps, collective_id)

        matrix = lambda t: t.reshape(-1, t.shape[2])
        wg0, wu0 = map(matrix, call(None, (1,), [], [], (), 2, "gather", Gather((w_gate, w_up), (0, 0)), (0,) * 5, 0))
        late, wg0 = lax.optimization_barrier((w_down[1], wg0))
        wd1 = whole(late)

        a0 = normed(x)
        swish0, slope0, p0, wd0, wg1, wu1 = call(
            forward_kernel, both, [rows(d), cols, cols],
            [((t, ff), f32, *tile), ((t, ff), f32, *tile), ((t, ff), bf16, *tile)], (a0, wg0, wu0), 2, "forward",
            Gather((w_down, w_gate, w_up), (0, 1, 1)), (0, 1, 3, 7, -10), 1,
        )
        wd0, wg1, wu1 = matrix(wd0), matrix(wg1), matrix(wu1)
        h1, a1 = call(
            down_kernel, (t // bh,), [slab(ff), full(wd0), slab(d)], [((t, d), bf16, *slab(d))] * 2, (p0, wd0, x), 1, "down"
        )
        p1, by_gate1, by_up1 = call(
            turn_kernel, both, [rows(d), rows(d), cols, cols, down], [((t, ff), bf16, *tile)] * 3,
            (a1, dy, wg1, wu1, wd1), 3, "turn",
        )
        g_gate1, g_up1 = weight(a1, by_gate1, "g_gate"), weight(a1, by_up1, "g_up")
        p1, _ = lax.optimization_barrier((p1, g_up1))
        g_down1 = weight(p1, dy, "g_down")
        g_gate1, g_up1 = (lax.psum_scatter(g, "dp", scatter_dimension=0, tiled=True) for g in (g_gate1, g_up1))
        by_h1, g_down1 = to_input(by_gate1, by_up1, wg1, wu1, h1, dy, Scatter((g_down1,)), (0, 1, 2, 3, -4), 2)
        g_down0 = weight(p0, by_h1, "g_down")
        by_gate0, by_up0, g_down0 = call(
            product_kernel, both, [rows(d), down, tile, tile], [((t, ff), bf16, *tile)] * 2, (by_h1, wd0, swish0, slope0), 1,
            "product", Scatter((g_down0,)), (0, 2, 5, 7, -10), 3,
        )
        terms0 = [weight(a0, by_gate0, "g_gate"), weight(a0, by_up0, "g_up")]
        by_x, g_gate0, g_up0 = to_input(by_gate0, by_up0, wg0, wu0, x, by_h1, Scatter(terms0), (0, 1, 3, -4, -4), 4)
        grads0, grads1 = (g_gate0, g_up0, g_down0), (g_gate1, g_up1, g_down1)
        return (by_x[None], *(jnp.stack([g0, g1]) for g0, g1 in zip(grads0, grads1)))

    tok = P(("rep", "dp"), None, None)
    w = P(None, "dp", None)
    g = P("rep", "dp", None)
    return jax.shard_map(step, mesh=mesh, in_specs=(tok, tok, w, w, w), out_specs=(tok, g, g, g), check_vma=False)
```
